128 devices in a mesh: head: 4 (over z_lo, core), seq: 32 (over z_hi, x, y).
Axes of the slice: x: 4, y: 4, z: 4 (z_hi: 2, z_lo: 2; z = z_hi * 2 + z_lo), core: 2. Of those that a mesh axis runs over, the one named last changes fastest.
Arguments:
- queries: bfloat16 [16384, 4096], P('seq', 'head'), may hold values from -512 to 512
- keys: bfloat16 [16384, 2048], P('seq', 'head'), may hold values from -8 to 8
- values: bfloat16 [16384, 2048], P('seq', 'head'), may hold values from -6 to 6
- episode: int32 [16384], replicated, may hold values from 0 to 7, never falling along the last dimension, each value on 1 to 4096 neighbouring positions
- out_weight: bfloat16 [4096, 4608], P('head'), may hold values from -0.375 to 0.375
Outputs:
- projected: bfloat16 [16384, 4608], P('seq', 'head')
The draws below stay inside these ranges and needn't reach their ends.
Inputs may be any that keep to these rules, and one draw needn't show every extreme that they name: episode numbers never fall along the trajectory.
All inputs are finite; a program needn't handle non-finite values.
Results may differ from the reference program's by a relative error of at most 0.015.
Values may be sent and summed in bfloat16 or wider, within the bound.
A program may use at most 192 MiB of HBM per device.

```python
import math
import jax
import jax.numpy as jnp
import numpy as np
from jax import lax

D = 4608
HEADS = 32
KV_HEADS = 16
HEAD_DIM = 128
WINDOW = 4096
S_DEV = 512
SEGMENTS = 8
TOKENS = 16384
N_HEAD = 4


def draw_common(key):
    key_q, key_k = jax.random.split(key, 2)
    base_k = jnp.clip(jax.random.normal(key_k, (TOKENS, KV_HEADS, HEAD_DIM), jnp.float32), -6.0, 6.0)
    base_q = 2.5 * jnp.clip(jax.random.normal(key_q, (TOKENS, HEADS, HEAD_DIM), jnp.float32), -6.0, 6.0)
    keys_out = base_k
    queries_out = base_q
    return (queries_out.reshape(TOKENS, HEADS * HEAD_DIM), keys_out.reshape(TOKENS, KV_HEADS * HEAD_DIM))


def draw_queries(key, part):
    return draw_common(jax.random.fold_in(key, 7))[0].astype(jnp.bfloat16)


def draw_keys(key, part):
    return draw_common(jax.random.fold_in(key, 7))[1].astype(jnp.bfloat16)


def level_of(rng, dims, cuts, least, top_value):
    factor_of = 1.0
    for axis_at, shards_of in cuts:
        heights = jax.random.uniform(jax.random.fold_in(jax.random.fold_in(rng, 6), axis_at), (shards_of,), jnp.float32, least / len(cuts), top_value / len(cuts))
        factor_of = factor_of * jnp.repeat(jnp.exp(heights), dims[axis_at] // shards_of).reshape((-1,) + (1,) * (len(dims) - 1 - axis_at))
    return factor_of


def profile(amount, total, bound, skew):
    loads = [(1 << 20) // math.isqrt(standing ** skew) + 1 for standing in range(2, amount + 1)]
    rest, given = total - bound - (amount - 1), [1] * (amount - 1)
    while rest > 0:
        candidates = [i for i in range(amount - 1) if given[i] < bound]
        pool, left = sum([loads[i] for i in candidates]), rest
        for i in candidates:
            more = min(bound - given[i], max(1, left * loads[i] // pool), rest)
            given[i] = given[i] + more
            rest = rest - more
    return np.array([bound] + given)


def uneven_parts(own_key, amount, total, bound, skew):
    if amount == 2:
        one = jax.random.randint(own_key, (), max(1, total - bound), min(bound, total - 1) + 1)
        return jnp.stack([one, total - one])
    sizes = jnp.asarray(profile(amount, total, bound, skew), jnp.int32)
    twos = (amount - 1) // 2
    giver, sink = sizes[1:1 + 2 * twos:2], sizes[2:2 + 2 * twos:2]
    margin = jnp.minimum(giver - 1, bound - sink)
    shifted = jax.random.randint(jax.random.fold_in(own_key, 1), (twos,), 0, 1 << 20) % (margin + 1)
    sizes = sizes.at[1:1 + 2 * twos:2].set(giver - shifted).at[2:2 + 2 * twos:2].set(sink + shifted)
    return sizes[jax.random.permutation(jax.random.fold_in(own_key, 2), amount)]


def centred(own_key, dims, deviation, reach, pieces=(), held_as=jnp.bfloat16):
    level = level_of(own_key, dims, pieces, -0.22, 0.18) if pieces else 1.0
    result = jax.random.normal(own_key, dims, jnp.float32) * deviation * level
    return jnp.minimum(jnp.maximum(result, -reach), reach).astype(held_as)


def setup_inputs(seed: int = 0) -> dict:
    splits = jax.random.split(jax.random.key(seed), 6)
    queries = draw_queries(jax.random.fold_in(splits[5], 71), 0)
    keys = draw_keys(jax.random.fold_in(splits[5], 71), 0)
    values = centred(splits[2], (TOKENS, KV_HEADS * HEAD_DIM), 1.0, 6.0, ((0, 32), (1, 4)))
    episode = jnp.searchsorted(jnp.cumsum(uneven_parts(splits[3], SEGMENTS, TOKENS, TOKENS // 4, 1)), jnp.arange(TOKENS), side="right").astype(jnp.int32)
    out_weight = centred(splits[4], (HEADS * HEAD_DIM, D), (HEAD_DIM * HEADS // 16) ** -0.5, 0.375, ((0, 4),))
    return {"queries": queries, "keys": keys, "values": values, "episode": episode, "out_weight": out_weight}


query_scale = 1.0 / 12.0


def reference(queries, keys, values, episode, out_weight):
    ratio = HEADS // KV_HEADS
    kv_width = KV_HEADS * HEAD_DIM
    span = WINDOW + S_DEV
    padded_keys = jnp.concatenate([jnp.zeros((WINDOW, kv_width), keys.dtype), keys], axis=0)
    padded_values = jnp.concatenate([jnp.zeros((WINDOW, kv_width), values.dtype), values], axis=0)
    padded_ids = jnp.concatenate([jnp.full((WINDOW,), -1, jnp.int32), episode.astype(jnp.int32)])

    def one_block(index):
        begin = (index * S_DEV).astype(jnp.int32)
        q_block = lax.dynamic_slice_in_dim(queries, begin, S_DEV, 0).astype(jnp.float32)
        q_block = q_block.reshape(S_DEV, KV_HEADS, ratio, HEAD_DIM)
        k_block = lax.dynamic_slice_in_dim(padded_keys, begin, span, 0).astype(jnp.float32)
        k_block = k_block.reshape(span, KV_HEADS, HEAD_DIM)
        v_block = lax.dynamic_slice_in_dim(padded_values, begin, span, 0).astype(jnp.float32)
        v_block = v_block.reshape(span, KV_HEADS, HEAD_DIM)
        ids_keys = lax.dynamic_slice_in_dim(padded_ids, begin, span, 0)
        ids_query = lax.dynamic_slice_in_dim(episode.astype(jnp.int32), begin, S_DEV, 0)
        q_pos = WINDOW + jnp.arange(S_DEV, dtype=jnp.int32)
        k_pos = jnp.arange(span, dtype=jnp.int32)
        visible = (k_pos[None, :] <= q_pos[:, None]) & (k_pos[None, :] > q_pos[:, None] - WINDOW)
        visible = visible & (ids_keys[None, :] == ids_query[:, None])
        scores = jnp.einsum("sgrd,tgd->grst", q_block, k_block, precision=lax.Precision.HIGHEST) * query_scale
        scores = jnp.where(visible[None, None], scores, jnp.float32(-1e30))
        top = jnp.max(scores, axis=-1, keepdims=True)
        expd = jnp.exp(scores - top)
        weights = (expd / jnp.sum(expd, axis=-1, keepdims=True)).astype(jnp.bfloat16).astype(jnp.float32)
        mixed = jnp.einsum("grst,tgd->sgrd", weights, v_block, precision=lax.Precision.HIGHEST)
        return mixed.astype(jnp.bfloat16).reshape(S_DEV, HEADS * HEAD_DIM)

    blocks = lax.map(one_block, jnp.arange(TOKENS // S_DEV, dtype=jnp.int32))
    attended = blocks.reshape(TOKENS, HEADS * HEAD_DIM)
    width = HEADS * HEAD_DIM // N_HEAD
    total = jnp.zeros((TOKENS, D), jnp.float32)
    for group in range(N_HEAD):
        piece = jnp.dot(attended[:, group * width:(group + 1) * width], out_weight[group * width:(group + 1) * width], preferred_element_type=jnp.float32)
        piece = lax.optimization_barrier(piece.astype(jnp.bfloat16))
        total = total + piece.astype(jnp.float32)
    return total.astype(jnp.bfloat16)
```

```python
import functools

import jax
import jax.numpy as jnp
from jax import lax
from jax.experimental import pallas as pl
from jax.experimental.pallas import tpu as pltpu
from jax.sharding import PartitionSpec as P

WINDOW = 4096
DH = 128
ROWS = 512
LINE = 4
SCALE2 = 1.4426950408889634 / 12.0
MESH = pl.DeviceIdType.MESH
VM = pltpu.VMEM
DMA = pltpu.SemaphoreType.DMA


def place():
    s = lax.axis_index("seq")
    h = lax.axis_index("head")
    p = lax.div(s, 16)
    x = lax.rem(lax.div(s, 4), 4)
    y = lax.rem(s, 4)
    return s, h, p, x, y


def at(s, h):
    return {"seq": s, "head": h}


def remote(src, dst, send, recv, dev):
    return pltpu.make_async_remote_copy(
        src_ref=src, dst_ref=dst, send_sem=send, recv_sem=recv, device_id=dev, device_id_type=MESH
    )


def greet(devs):
    barrier = pltpu.get_barrier_semaphore()
    for dev in devs:
        pl.semaphore_signal(barrier, inc=1, device_id=dev, device_id_type=MESH)
    pl.semaphore_wait(barrier, len(devs))


ORDER = (0, 1, 3, 2)


def exchange_kernel(q, k, v, qbuf, kvbuf, cross, relay, l_sem, sy, ry, sq, rq, s1, r1, s2, r2, sc, rc, sr, rr):
    s, h, p, x, y = place()
    base = s - y
    x_next = p * 16 + lax.rem(x + 1, 4) * 4 + y
    x_prev = p * 16 + lax.rem(x + 3, 4) * 4 + y
    z_other = (1 - p) * 16 + x * 4 + y
    ys = {d: base + lax.rem(y + d, 4) for d in range(1, 4)}
    greet([at(ys[d], h) for d in (1, 2, 3)] + [at(t, h) for t in (x_next, x_prev, z_other)])

    local = []
    for i, src in enumerate((k, v)):
        local.append(pltpu.make_async_copy(src.at[:, pl.ds(y * DH, DH)], kvbuf.at[2, y, i], l_sem.at[i]))
        local[-1].start()
    q_local = pltpu.make_async_copy(q.at[:, pl.ds(y * 2 * DH, 2 * DH)], qbuf.at[y], l_sem.at[2])
    q_local.start()
    y_copies = []
    for d in ORDER[1:]:
        to = lax.rem(y + d, 4)
        for i, src in enumerate((k, v)):
            c = remote(src.at[:, pl.ds(to * DH, DH)], kvbuf.at[2, y, i], sy.at[d, i], ry.at[d, i], at(ys[d], h))
            c.start()
            y_copies.append(c)
    for d in ORDER[1:]:
        to = lax.rem(y + d, 4)
        c = remote(q.at[:, pl.ds(to * 2 * DH, 2 * DH)], qbuf.at[y], sq.at[d], rq.at[d], at(ys[d], h))
        c.start()
        y_copies.append(c)

    def own_out(b, d, i):
        return remote(kvbuf.at[2, b, i], kvbuf.at[1, b, i], s1.at[d, i], r1.at[d, i], at(x_next, h))

    def own_cross(b, d, i):
        return remote(kvbuf.at[2, b, i], cross.at[b, i], sc.at[d, i], rc.at[d, i], at(z_other, h))

    def forward(b, d, i):
        return remote(kvbuf.at[1, b, i], kvbuf.at[0, b, i], s2.at[d, i], r2.at[d, i], at(x_next, h))

    def cross_next(b, d, i):
        return remote(cross.at[b, i], kvbuf.at[1, b, i], s1.at[d, i], r1.at[d, i], at(x_next, h))

    def cross_back(b, d, i):
        return remote(cross.at[b, i], relay.at[b, i], sr.at[d, i], rr.at[d, i], at(x_prev, h))

    def relay_back(b, d, i):
        return remote(relay.at[b, i], kvbuf.at[0, b, i], sr.at[d, i], r2.at[d, i], at(x_prev, h))

    for d in ORDER:
        b = lax.rem(y - d + 4, 4)
        for i in range(2):
            if d == 0:
                local[i].wait()
            else:
                remote(k.at[:, pl.ds(0, DH)], kvbuf.at[2, b, i], sy.at[d, i], ry.at[d, i], at(ys[d], h)).wait_recv()

            @pl.when(jnp.logical_and(p == 0, x >= 2))
            def _():
                own_cross(b, d, i).start()

            @pl.when(x < 3)
            def _():
                own_out(b, d, i).start()

    for d in ORDER:
        b = lax.rem(y - d + 4, 4)
        for i in range(2):

            @pl.when(jnp.logical_and(p == 1, x >= 2))
            def _():
                own_cross(b, d, i).wait_recv()

            @pl.when(jnp.logical_and(p == 1, x == 3))
            def _():
                cross_next(b, d, i).start()

            @pl.when(jnp.logical_and(p == 1, x == 2))
            def _():
                cross_back(b, d, i).start()

            @pl.when(x + p * 4 >= 1)
            def _():
                own_out(b, d, i).wait_recv()

            @pl.when(jnp.logical_or(jnp.logical_or(x == 1, x == 2), jnp.logical_and(p == 1, x == 0)))
            def _():
                forward(b, d, i).start()

            @pl.when(jnp.logical_and(p == 1, x == 1))
            def _():
                cross_back(b, d, i).wait_recv()
                relay_back(b, d, i).start()

    q_local.wait()
    for c in y_copies[6:]:
        c.wait_recv()
    for c in y_copies:
        c.wait_send()
    for d in ORDER:
        b = lax.rem(y - d + 4, 4)
        for i in range(2):

            @pl.when(x + p * 4 >= 2)
            def _():
                forward(b, d, i).wait_recv()

            @pl.when(jnp.logical_or(x < 3, p == 1))
            def _():
                own_out(b, d, i).wait_send()

            @pl.when(jnp.logical_and(p == 0, x >= 2))
            def _():
                own_cross(b, d, i).wait_send()

            @pl.when(jnp.logical_or(jnp.logical_or(x == 1, x == 2), jnp.logical_and(p == 1, x == 0)))
            def _():
                forward(b, d, i).wait_send()

            @pl.when(jnp.logical_and(p == 1, jnp.logical_or(x == 1, x == 2)))
            def _():
                relay_back(b, d, i).wait_send()


def exchange(q, k, v):
    pair = DMA((4, 2))
    return pl.pallas_call(
        exchange_kernel,
        out_shape=(
            jax.ShapeDtypeStruct((LINE, ROWS, 2 * DH), jnp.bfloat16),
            jax.ShapeDtypeStruct((3, LINE, 2, ROWS, DH), jnp.bfloat16),
        ),
        in_specs=[pl.BlockSpec(memory_space=pl.ANY)] * 3,
        out_specs=(pl.BlockSpec(memory_space=VM), pl.BlockSpec(memory_space=VM)),
        scratch_shapes=[
            VM((LINE, 2, ROWS, DH), jnp.bfloat16),
            VM((LINE, 2, ROWS, DH), jnp.bfloat16),
            DMA((3,)),
            pair, pair, DMA((4,)), DMA((4,)),
            pair, pair, pair, pair, pair, pair, pair, pair,
        ],
        compiler_params=pltpu.CompilerParams(collective_id=0, has_side_effects=True),
        name="exchange",
    )(q, k, v)


TQ = 256
TK = 512
SUB = 128


def attention_kernel(first, q, kv, lo, o, m_ref, acc_ref):
    ones = jnp.ones((TK, DH), jnp.bfloat16)

    def tile(qi, t, causal):
        yb, r0 = lax.div(qi, 2), lax.rem(qi, 2) * TQ
        g, b = lax.div(t, 4), lax.rem(t, 4)
        kt = kv[g, b, 0]
        vt = jnp.concatenate([kv[g, b, 1], ones], axis=1)
        col = t * TK + lax.broadcasted_iota(jnp.int32, (SUB, TK), 1)
        for part in range(TQ // SUB):
            lo_col = lo[pl.ds(qi * TQ + part * SUB, SUB), :]
            ok = col >= lo_col
            if causal:
                row = 2 * 2048 + qi * TQ + part * SUB + lax.broadcasted_iota(jnp.int32, (SUB, TK), 0)
                ok = jnp.logical_and(ok, col <= row)
            for head in range(2):
                at_row = head * TQ + part * SUB
                qt = q[yb, pl.ds(r0 + part * SUB, SUB), head * DH : (head + 1) * DH]
                sc = lax.dot_general(qt, kt, (((1,), (1,)), ((), ())), preferred_element_type=jnp.float32)
                sc = jnp.where(ok, sc, jnp.float32(-1e30))
                m_old = m_ref[at_row : at_row + SUB, :]
                m_new = jnp.maximum(m_old, jnp.max(sc, axis=1, keepdims=True))
                pr = jnp.exp2((sc - m_new[:, 0:1]) * SCALE2).astype(jnp.bfloat16)
                alpha = jnp.exp2((m_old - m_new) * SCALE2)
                upd = jnp.dot(pr, vt, preferred_element_type=jnp.float32)
                acc = acc_ref[at_row : at_row + SUB, :]
                acc_ref[at_row : at_row + SUB, :] = acc * jnp.concatenate([alpha, alpha], axis=1) + upd
                m_ref[at_row : at_row + SUB, :] = m_new

    def q_tile(qi, _):
        m_ref[...] = jnp.full(m_ref.shape, -1e30, jnp.float32)
        acc_ref[...] = jnp.zeros(acc_ref.shape, jnp.float32)
        last = 8 + lax.div(qi, 2)

        def step(t, _):
            tile(qi, t, False)
            return 0

        lax.fori_loop(lax.div(first[qi], TK), last, step, 0)
        tile(qi, last, True)
        yb, r0 = lax.div(qi, 2), lax.rem(qi, 2) * TQ
        for head in range(2):
            part = acc_ref[head * TQ : (head + 1) * TQ, :]
            o[yb, pl.ds(r0, TQ), head * DH : (head + 1) * DH] = (part[:, :DH] / part[:, DH:]).astype(jnp.bfloat16)
        return 0

    lax.fori_loop(0, 8, q_tile, 0)


def attention(q, kv, lo):
    first = lo[::TQ]
    return pl.pallas_call(
        attention_kernel,
        out_shape=jax.ShapeDtypeStruct((LINE, ROWS, 2 * DH), jnp.bfloat16),
        in_specs=[pl.BlockSpec(memory_space=pltpu.SMEM)] + [pl.BlockSpec(memory_space=VM)] * 3,
        out_specs=pl.BlockSpec(memory_space=VM),
        scratch_shapes=[VM((2 * TQ, DH), jnp.float32), VM((2 * TQ, 2 * DH), jnp.float32)],
        name="attention",
    )(first, q, kv, lo[:, None])


CH = 128
NCH = ROWS // CH
FQ = 1152


def project_kernel(o, w_hbm, out, w, obuf, mine, keep, csend, crecv, zsend, zrecv, w_sem, so, ro, scs, rcs, szs, rzs):
    s, h, p, x, y = place()
    base = s - y
    core, zl = lax.rem(h, 2), lax.div(h, 2)
    mate, zmate = zl * 2 + (1 - core), (1 - zl) * 2 + core
    ys = {d: base + lax.rem(y + d, 4) for d in range(1, 4)}
    loads = []
    for j in range(4):
        c = pltpu.make_async_copy(w_hbm.at[pl.ds(j * 256, 256)], w.at[pl.ds(j * 256, 256)], w_sem.at[j])
        c.start()
        loads.append(c)
    greet([at(ys[d], h) for d in (1, 2, 3)] + [at(s, mate), at(s, zmate)])

    def o_copy(c, d):
        to = lax.rem(y + d, 4)
        return remote(o.at[to, pl.ds(c * CH, CH)], obuf.at[y, pl.ds(c * CH, CH)], so.at[c, d], ro.at[c, d], at(ys[d], h))

    for c in range(NCH):
        for d in ORDER[1:]:
            o_copy(c, d).start()
    obuf[y] = o[y]
    for c in loads:
        c.wait()

    def core_copy(c, j):
        return remote(csend.at[c, j], crecv.at[c, j], scs.at[c, j], rcs.at[c, j], at(s, mate))

    def z_copy(c):
        return remote(zsend.at[c], zrecv.at[c], szs.at[c], rzs.at[c], at(s, zmate))

    def compute(c):
        for d in ORDER[1:]:
            o_copy(c, d).wait_recv()
        a = jnp.concatenate([obuf[j, c * CH : (c + 1) * CH, :] for j in range(4)], axis=1)
        for j in range(2):
            f = (j * 2 + (1 - core)) * FQ
            csend[c, j] = jnp.dot(a, w[:, pl.ds(pl.multiple_of(f, 128), FQ)], preferred_element_type=jnp.float32).astype(jnp.bfloat16)
        for j in range(2):
            core_copy(c, j).start()
        for j in range(2):
            f = (j * 2 + core) * FQ
            mine[c % 2, j] = jnp.dot(a, w[:, pl.ds(pl.multiple_of(f, 128), FQ)], preferred_element_type=jnp.float32)

    def reduce_core(c):
        for j in range(2):
            core_copy(c, j).wait_recv()
        zsend[c] = (mine[c % 2, 1 - zl] + crecv[c, 1 - zl].astype(jnp.float32)).astype(jnp.bfloat16)
        keep[c] = mine[c % 2, zl] + crecv[c, zl].astype(jnp.float32)
        z_copy(c).start()

    for c in range(NCH):
        compute(c)
        if c >= 1:
            reduce_core(c - 1)
    reduce_core(NCH - 1)
    for c in range(NCH):
        z_copy(c).wait_recv()
        out[c * CH : (c + 1) * CH, :] = (keep[c] + zrecv[c].astype(jnp.float32)).astype(jnp.bfloat16)
    for c in range(NCH):
        z_copy(c).wait_send()
        for j in range(2):
            core_copy(c, j).wait_send()
        for d in ORDER[1:]:
            o_copy(c, d).wait_send()


def project(o, w):
    bf, f32 = jnp.bfloat16, jnp.float32
    return pl.pallas_call(
        project_kernel,
        out_shape=jax.ShapeDtypeStruct((ROWS, FQ), bf),
        in_specs=[pl.BlockSpec(memory_space=VM), pl.BlockSpec(memory_space=pl.ANY)],
        out_specs=pl.BlockSpec(memory_space=VM),
        scratch_shapes=[
            VM((1024, 4 * FQ), bf),
            VM((LINE, ROWS, 2 * DH), bf),
            VM((2, 2, CH, FQ), f32),
            VM((NCH, CH, FQ), f32),
            VM((NCH, 2, CH, FQ), bf),
            VM((NCH, 2, CH, FQ), bf),
            VM((NCH, CH, FQ), bf),
            VM((NCH, CH, FQ), bf),
            DMA((4,)),
            DMA((NCH, 4)), DMA((NCH, 4)),
            DMA((NCH, 2)), DMA((NCH, 2)),
            DMA((NCH,)), DMA((NCH,)),
        ],
        compiler_params=pltpu.CompilerParams(collective_id=1, has_side_effects=True),
        name="project",
    )(o, w)


def body(queries, keys, values, episode, out_weight):
    group = lax.div(lax.axis_index("seq"), LINE)
    rows = LINE * ROWS
    starts = jnp.sum((episode[None, :] < jnp.arange(8, dtype=jnp.int32)[:, None]).astype(jnp.int32), axis=1)
    ids = lax.dynamic_slice_in_dim(episode, group * rows, rows, 0)
    begin = jnp.sum(jnp.where(ids[:, None] == jnp.arange(8, dtype=jnp.int32)[None, :], starts[None, :], 0), axis=1)
    pos = group * rows + jnp.arange(rows, dtype=jnp.int32)
    lo = jnp.maximum(begin, pos - (WINDOW - 1)) - (group * rows - WINDOW)
    q, kv = exchange(queries, keys, values)
    o = attention(q, kv, lo)
    return project(o, out_weight)


def solution(mesh):
    placed = (P("seq", "head"), P("seq", "head"), P("seq", "head"), P(), P("head", None))
    return jax.shard_map(body, mesh=mesh, in_specs=placed, out_specs=P("seq", "head"), check_vma=False)
```

```python
import functools

import jax
import jax.numpy as jnp
from jax import lax
from jax.experimental import pallas as pl
from jax.experimental.pallas import tpu as pltpu
from jax.sharding import PartitionSpec as P

WINDOW = 4096
DH = 128
ROWS = 512
LINE = 4
SCALE2 = 1.4426950408889634 / 12.0
MESH = pl.DeviceIdType.MESH
VM = pltpu.VMEM
DMA = pltpu.SemaphoreType.DMA


def place():
    s = lax.axis_index("seq")
    h = lax.axis_index("head")
    p = lax.div(s, 16)
    x = lax.rem(lax.div(s, 4), 4)
    y = lax.rem(s, 4)
    return s, h, p, x, y


def at(s, h):
    return {"seq": s, "head": h}


def remote(src, dst, send, recv, dev):
    return pltpu.make_async_remote_copy(
        src_ref=src, dst_ref=dst, send_sem=send, recv_sem=recv, device_id=dev, device_id_type=MESH
    )


def greet(devs):
    barrier = pltpu.get_barrier_semaphore()
    for dev in devs:
        pl.semaphore_signal(barrier, inc=1, device_id=dev, device_id_type=MESH)
    pl.semaphore_wait(barrier, len(devs))


ORDER = (0, 1, 3, 2)


def exchange_kernel(q, k, v, qbuf, kvbuf, cross, relay, l_sem, sy, ry, sq, rq, s1, r1, s2, r2, sc, rc, sr, rr):
    s, h, p, x, y = place()
    base = s - y
    x_next = p * 16 + lax.rem(x + 1, 4) * 4 + y
    x_prev = p * 16 + lax.rem(x + 3, 4) * 4 + y
    z_other = (1 - p) * 16 + x * 4 + y
    ys = {d: base + lax.rem(y + d, 4) for d in range(1, 4)}
    greet([at(ys[d], h) for d in (1, 2, 3)] + [at(t, h) for t in (x_next, x_prev, z_other)])

    local = []
    for i, src in enumerate((k, v)):
        local.append(pltpu.make_async_copy(src.at[:, pl.ds(y * DH, DH)], kvbuf.at[2, y, i], l_sem.at[i]))
        local[-1].start()
    q_local = pltpu.make_async_copy(q.at[:, pl.ds(y * 2 * DH, 2 * DH)], qbuf.at[y], l_sem.at[2])
    q_local.start()
    y_copies = []
    for d in ORDER[1:]:
        to = lax.rem(y + d, 4)
        for i, src in enumerate((k, v)):
            c = remote(src.at[:, pl.ds(to * DH, DH)], kvbuf.at[2, y, i], sy.at[d, i], ry.at[d, i], at(ys[d], h))
            c.start()
            y_copies.append(c)
    for d in ORDER[1:]:
        to = lax.rem(y + d, 4)
        c = remote(q.at[:, pl.ds(to * 2 * DH, 2 * DH)], qbuf.at[y], sq.at[d], rq.at[d], at(ys[d], h))
        c.start()
        y_copies.append(c)

    def own_out(b, d, i):
        return remote(kvbuf.at[2, b, i], kvbuf.at[1, b, i], s1.at[d, i], r1.at[d, i], at(x_next, h))

    def own_cross(b, d, i):
        return remote(kvbuf.at[2, b, i], cross.at[b, i], sc.at[d, i], rc.at[d, i], at(z_other, h))

    def forward(b, d, i):
        return remote(kvbuf.at[1, b, i], kvbuf.at[0, b, i], s2.at[d, i], r2.at[d, i], at(x_next, h))

    def cross_next(b, d, i):
        return remote(cross.at[b, i], kvbuf.at[1, b, i], s1.at[d, i], r1.at[d, i], at(x_next, h))

    def cross_back(b, d, i):
        return remote(cross.at[b, i], relay.at[b, i], sr.at[d, i], rr.at[d, i], at(x_prev, h))

    def relay_back(b, d, i):
        return remote(relay.at[b, i], kvbuf.at[0, b, i], sr.at[d, i], r2.at[d, i], at(x_prev, h))

    for d in ORDER:
        b = lax.rem(y - d + 4, 4)
        for i in range(2):
            if d == 0:
                local[i].wait()
            else:
                remote(k.at[:, pl.ds(0, DH)], kvbuf.at[2, b, i], sy.at[d, i], ry.at[d, i], at(ys[d], h)).wait_recv()

            @pl.when(jnp.logical_and(p == 0, x >= 2))
            def _():
                own_cross(b, d, i).start()

            @pl.when(x < 3)
            def _():
                own_out(b, d, i).start()

    for d in ORDER:
        b = lax.rem(y - d + 4, 4)
        for i in range(2):

            @pl.when(jnp.logical_and(p == 1, x >= 2))
            def _():
                own_cross(b, d, i).wait_recv()

            @pl.when(jnp.logical_and(p == 1, x == 3))
            def _():
                cross_next(b, d, i).start()

            @pl.when(jnp.logical_and(p == 1, x == 2))
            def _():
                cross_back(b, d, i).start()

            @pl.when(x + p * 4 >= 1)
            def _():
                own_out(b, d, i).wait_recv()

            @pl.when(jnp.logical_or(jnp.logical_or(x == 1, x == 2), jnp.logical_and(p == 1, x == 0)))
            def _():
                forward(b, d, i).start()

            @pl.when(jnp.logical_and(p == 1, x == 1))
            def _():
                cross_back(b, d, i).wait_recv()
                relay_back(b, d, i).start()

    q_local.wait()
    for c in y_copies[6:]:
        c.wait_recv()
    for c in y_copies:
        c.wait_send()
    for d in ORDER:
        b = lax.rem(y - d + 4, 4)
        for i in range(2):

            @pl.when(x + p * 4 >= 2)
            def _():
                forward(b, d, i).wait_recv()

            @pl.when(jnp.logical_or(x < 3, p == 1))
            def _():
                own_out(b, d, i).wait_send()

            @pl.when(jnp.logical_and(p == 0, x >= 2))
            def _():
                own_cross(b, d, i).wait_send()

            @pl.when(jnp.logical_or(jnp.logical_or(x == 1, x == 2), jnp.logical_and(p == 1, x == 0)))
            def _():
                forward(b, d, i).wait_send()

            @pl.when(jnp.logical_and(p == 1, jnp.logical_or(x == 1, x == 2)))
            def _():
                relay_back(b, d, i).wait_send()


def exchange(q, k, v):
    pair = DMA((4, 2))
    return pl.pallas_call(
        exchange_kernel,
        out_shape=(
            jax.ShapeDtypeStruct((LINE, ROWS, 2 * DH), jnp.bfloat16),
            jax.ShapeDtypeStruct((3, LINE, 2, ROWS, DH), jnp.bfloat16),
        ),
        in_specs=[pl.BlockSpec(memory_space=pl.ANY)] * 3,
        out_specs=(pl.BlockSpec(memory_space=VM), pl.BlockSpec(memory_space=VM)),
        scratch_shapes=[
            VM((LINE, 2, ROWS, DH), jnp.bfloat16),
            VM((LINE, 2, ROWS, DH), jnp.bfloat16),
            DMA((3,)),
            pair, pair, DMA((4,)), DMA((4,)),
            pair, pair, pair, pair, pair, pair, pair, pair,
        ],
        compiler_params=pltpu.CompilerParams(collective_id=0, has_side_effects=True),
        name="exchange",
    )(q, k, v)


TK = 512
HALF = 256
VROWS = DH + 16
FAR = -1e30


def turn_queries(q, ids, qt):
    for yb in range(LINE):
        for half in range(2):
            e = lax.broadcasted_iota(jnp.int32, (DH, HALF), 0)
            hidden = jnp.logical_and(e != ids[yb * 2 + half : yb * 2 + half + 1, :], e <= 8)
            hidden = jnp.where(hidden, jnp.float32(FAR), jnp.float32(0)).astype(jnp.bfloat16)
            for head in range(2):
                part = q[yb, half * HALF : (half + 1) * HALF, head * DH : (head + 1) * DH]
                qt[yb, head * 2 + half, 0:DH, :] = part.T
                qt[yb, head * 2 + half, DH:, :] = hidden


def turn_values(vt, t, block):
    vt[t, 0:DH, :] = block.T
    vt[t, DH:VROWS, :] = jnp.ones((VROWS - DH, TK), jnp.bfloat16)


def tile(yb, t, k, marks, qt, vt, m_ref, acc_ref, s_refs, p_refs, kind):
    units = []
    for head in range(2):
        for half in range(2):
            span = {"full": (0, TK), "causal": (0, HALF * (half + 1)), "window": (HALF * half, TK)}[kind]
            units.append((head * 2 + half, half, span))
    alphas = [None] * 4

    def scores(n):
        u, half, (a, b) = units[n]
        kk = jnp.concatenate([k[a:b, :], marks[t, a:b, :]], axis=1)
        s_refs[n % 2][a:b, :] = jnp.dot(kk, qt[yb, u], preferred_element_type=jnp.float32)

    def soft(n):
        u, half, (a, b) = units[n]
        sc = s_refs[n % 2][a:b, :]
        if kind != "full":
            key = a + lax.broadcasted_iota(jnp.int32, (b - a, HALF), 0)
            row = half * HALF + lax.broadcasted_iota(jnp.int32, (b - a, HALF), 1)
            ok = key <= row if kind == "causal" else key > row
            sc = jnp.where(ok, sc, jnp.float32(FAR))
        m_old = m_ref[yb, u]
        m_new = jnp.maximum(m_old, jnp.max(sc, axis=0, keepdims=True))
        p_refs[n % 2][a:b, :] = jnp.exp2((sc - m_new) * SCALE2).astype(jnp.bfloat16)
        alphas[n] = jnp.exp2((m_old - m_new) * SCALE2)
        m_ref[yb, u] = m_new

    def mix(n):
        u, half, (a, b) = units[n]
        upd = jnp.dot(vt[t, :, a:b], p_refs[n % 2][a:b, :], preferred_element_type=jnp.float32)
        acc_ref[yb, u] = acc_ref[yb, u] * alphas[n] + upd

    scores(0)
    for n in range(4):
        if n < 3:
            scores(n + 1)
        if n > 0:
            mix(n - 1)
        soft(n)
    mix(3)


def finish(yb, o, acc_ref):
    for half in range(2):
        for head in range(2):
            u = head * 2 + half
            inv = 1.0 / acc_ref[yb, u, DH : DH + 1, :]
            part = (acc_ref[yb, u, 0:DH, :] * inv).astype(jnp.bfloat16)
            o[yb, half * HALF : (half + 1) * HALF, head * DH : (head + 1) * DH] = part.T


def attention_kernel(first, q, kv, marks, ids, o, qt, vt, m_ref, acc_ref, s0, s1, p0, p1):
    turn_queries(q, ids, qt)
    for t in range(12):
        turn_values(vt, t, kv[t // 4, t % 4, 1])
    m_ref[...] = jnp.full(m_ref.shape, 2 * FAR, jnp.float32)
    acc_ref[...] = jnp.zeros(acc_ref.shape, jnp.float32)

    def q_block(yb, _):
        def one(t, kind):
            k = kv.at[lax.div(t, 4), lax.rem(t, 4), 0]
            tile(yb, t, k, marks, qt, vt, m_ref, acc_ref, (s0, s1), (p0, p1), kind)

        start = lax.div(first[yb], TK)

        @pl.when(start <= yb)
        def _():
            one(yb, "window")

        def step(t, _):
            one(t, "full")
            return 0

        lax.fori_loop(jnp.maximum(start, yb + 1), 8 + yb, step, 0)
        one(8 + yb, "causal")
        finish(yb, o, acc_ref)
        return 0

    lax.fori_loop(0, LINE, q_block, 0)


def attention(q, kv, marks, ids, first):
    f32, bf = jnp.float32, jnp.bfloat16
    return pl.pallas_call(
        attention_kernel,
        out_shape=jax.ShapeDtypeStruct((LINE, ROWS, 2 * DH), bf),
        in_specs=[pl.BlockSpec(memory_space=pltpu.SMEM)] + [pl.BlockSpec(memory_space=VM)] * 4,
        out_specs=pl.BlockSpec(memory_space=VM),
        scratch_shapes=[
            VM((LINE, 4, 2 * DH, HALF), bf),
            VM((12, VROWS, TK), bf),
            VM((LINE, 4, 1, HALF), f32),
            VM((LINE, 4, VROWS, HALF), f32),
            VM((TK, HALF), f32),
            VM((TK, HALF), f32),
            VM((TK, HALF), bf),
            VM((TK, HALF), bf),
        ],
        name="attention",
    )(first, q, kv, marks, ids)


CH = 128
NCH = ROWS // CH
FQ = 1152


def project_kernel(o, w_hbm, out, w, obuf, mine, keep, csend, crecv, zsend, zrecv, w_sem, so, ro, scs, rcs, szs, rzs):
    s, h, p, x, y = place()
    base = s - y
    core, zl = lax.rem(h, 2), lax.div(h, 2)
    mate, zmate = zl * 2 + (1 - core), (1 - zl) * 2 + core
    ys = {d: base + lax.rem(y + d, 4) for d in range(1, 4)}
    loads = []
    for j in range(4):
        c = pltpu.make_async_copy(w_hbm.at[pl.ds(j * 256, 256)], w.at[pl.ds(j * 256, 256)], w_sem.at[j])
        c.start()
        loads.append(c)
    greet([at(ys[d], h) for d in (1, 2, 3)] + [at(s, mate), at(s, zmate)])

    def o_copy(c, d):
        to = lax.rem(y + d, 4)
        return remote(o.at[to, pl.ds(c * CH, CH)], obuf.at[y, pl.ds(c * CH, CH)], so.at[c, d], ro.at[c, d], at(ys[d], h))

    for c in range(NCH):
        for d in ORDER[1:]:
            o_copy(c, d).start()
    obuf[y] = o[y]
    for c in loads:
        c.wait()

    def core_copy(c, j):
        return remote(csend.at[c, j], crecv.at[c, j], scs.at[c, j], rcs.at[c, j], at(s, mate))

    def z_copy(c):
        return remote(zsend.at[c], zrecv.at[c], szs.at[c], rzs.at[c], at(s, zmate))

    def compute(c):
        for d in ORDER[1:]:
            o_copy(c, d).wait_recv()
        a = jnp.concatenate([obuf[j, c * CH : (c + 1) * CH, :] for j in range(4)], axis=1)
        for j in range(2):
            f = (j * 2 + (1 - core)) * FQ
            csend[c, j] = jnp.dot(a, w[:, pl.ds(pl.multiple_of(f, 128), FQ)], preferred_element_type=jnp.float32).astype(jnp.bfloat16)
        for j in range(2):
            core_copy(c, j).start()
        for j in range(2):
            f = (j * 2 + core) * FQ
            mine[c % 2, j] = jnp.dot(a, w[:, pl.ds(pl.multiple_of(f, 128), FQ)], preferred_element_type=jnp.float32)

    def reduce_core(c):
        for j in range(2):
            core_copy(c, j).wait_recv()
        zsend[c] = (mine[c % 2, 1 - zl] + crecv[c, 1 - zl].astype(jnp.float32)).astype(jnp.bfloat16)
        keep[c] = mine[c % 2, zl] + crecv[c, zl].astype(jnp.float32)
        z_copy(c).start()

    for c in range(NCH):
        compute(c)
        if c >= 1:
            reduce_core(c - 1)
    reduce_core(NCH - 1)
    for c in range(NCH):
        z_copy(c).wait_recv()
        out[c * CH : (c + 1) * CH, :] = (keep[c] + zrecv[c].astype(jnp.float32)).astype(jnp.bfloat16)
    for c in range(NCH):
        z_copy(c).wait_send()
        for j in range(2):
            core_copy(c, j).wait_send()
        for d in ORDER[1:]:
            o_copy(c, d).wait_send()


def project(o, w):
    bf, f32 = jnp.bfloat16, jnp.float32
    return pl.pallas_call(
        project_kernel,
        out_shape=jax.ShapeDtypeStruct((ROWS, FQ), bf),
        in_specs=[pl.BlockSpec(memory_space=VM), pl.BlockSpec(memory_space=pl.ANY)],
        out_specs=pl.BlockSpec(memory_space=VM),
        scratch_shapes=[
            VM((1024, 4 * FQ), bf),
            VM((LINE, ROWS, 2 * DH), bf),
            VM((2, 2, CH, FQ), f32),
            VM((NCH, CH, FQ), f32),
            VM((NCH, 2, CH, FQ), bf),
            VM((NCH, 2, CH, FQ), bf),
            VM((NCH, CH, FQ), bf),
            VM((NCH, CH, FQ), bf),
            DMA((4,)),
            DMA((NCH, 4)), DMA((NCH, 4)),
            DMA((NCH, 2)), DMA((NCH, 2)),
            DMA((NCH,)), DMA((NCH,)),
        ],
        compiler_params=pltpu.CompilerParams(collective_id=1, has_side_effects=True),
        name="project",
    )(o, w)


def body(queries, keys, values, episode, out_weight):
    group = lax.div(lax.axis_index("seq"), LINE)
    rows = LINE * ROWS
    padded = jnp.concatenate([jnp.full((WINDOW,), 8, jnp.int32), episode])
    key_ids = lax.dynamic_slice_in_dim(padded, group * rows, WINDOW + rows, 0)
    ids = key_ids[WINDOW:]
    marks = (key_ids[:, None] == jnp.arange(DH, dtype=jnp.int32)[None, :]).astype(jnp.bfloat16)
    first = jnp.sum((key_ids[None, :] < ids[::ROWS, None]).astype(jnp.int32), axis=1)
    first = first + jnp.sum((key_ids == 8).astype(jnp.int32))
    q, kv = exchange(queries, keys, values)
    o = attention(q, kv, marks.reshape(12, TK, DH), ids.reshape(8, HALF), first)
    return project(o, out_weight)


def solution(mesh):
    placed = (P("seq", "head"), P("seq", "head"), P("seq", "head"), P(), P("head", None))
    return jax.shard_map(body, mesh=mesh, in_specs=placed, out_specs=P("seq", "head"), check_vma=False)
```
